32 devices in a mesh: tm: 8 (over y, x, core), panel: 4 (over z).
Axes of the slice: x: 2, y: 2, z: 4, core: 2. Of those that a mesh axis runs over, the one named last changes fastest.
Arguments:
- series: float32 [48, 2048], P(None, 'tm'), may hold values from -20 to 20, as said below
- start_block: float32 [18432, 64], P(('tm', 'panel')), may hold values from -6 to 6
Outputs:
- covariance: float32 [18432, 18432], P(('tm', 'panel'))
- basis: float32 [7, 18432, 64], P(None, ('tm', 'panel'))
- diag_blocks: float32 [6, 64, 64], replicated
- off_blocks: float32 [7, 64, 64], replicated
The draws below stay inside these ranges and needn't reach their ends.
Inputs may be any that keep to these rules, and one draw needn't show every extreme that they name: `series`: each channel has its own scale.
All inputs are finite; a program needn't handle non-finite values.
Results may differ from the reference program's by a relative error of at most 0.0003.
Values sent between devices are 32-bit elements; how exact they have to be, the bound alone decides.
A program may use at most 192 MiB of HBM per device.

```python
import math
import jax
import jax.numpy as jnp
from jax import lax

L = 48
M = 384
B = 64
ITERS = 6
NT = 2048
LM = 18432


def draw_series(key, part):
    scale_key = jax.random.fold_in(key, 11)
    noise_key = jax.random.fold_in(key, 12)
    scales = jnp.exp(jax.random.uniform(scale_key, (L, 1), jnp.float32, math.log(0.3), math.log(3.0)))
    noise = jnp.clip(jax.random.normal(noise_key, (L, NT), jnp.float32), -6.0, 6.0)
    return (scales * noise).astype(jnp.float32)


def block_levels(rng, dims, split, low, top_value):
    def one(axis_at, blocks):
        draws = jax.random.uniform(jax.random.fold_in(jax.random.fold_in(rng, 6), axis_at), (blocks,), jnp.float32, low / len(split), top_value / len(split))
        return jnp.repeat(jnp.exp(draws), dims[axis_at] // blocks).reshape((-1,) + (1,) * (len(dims) - axis_at - 1))

    factor_of = one(*split[0])
    for cut in split[1:]:
        factor_of = factor_of * one(*cut)
    return factor_of


def centred(rng, shape, scale, limit, split=(), kind=jnp.bfloat16):
    array = scale * jax.random.normal(rng, shape, jnp.float32)
    if split:
        array = array * block_levels(rng, shape, split, -0.22, 0.18)
    return jnp.clip(array, -limit, limit).astype(kind)


def setup_inputs(seed: int = 0) -> dict:
    seeds = jax.random.split(jax.random.key(seed), 3)
    return {
        "series": draw_series(jax.random.fold_in(seeds[2], 71), 0),
        "start_block": centred(seeds[1], (LM, B), 1.0, 6.0, ((0, 32),), jnp.float32),
    }


exact_precision = lax.Precision.HIGHEST

def lower_factor(gram_matrix):
    return jnp.linalg.cholesky(gram_matrix)

def reference(series, start_block):
    padded = jnp.concatenate([series, jnp.zeros((L, M), jnp.float32)], axis=1)

    def one_lag(lag_index):
        shifted = lax.dynamic_slice(padded, (jnp.int32(0), lag_index.astype(jnp.int32)), (L, NT))
        return jnp.dot(series.astype(jnp.float32), shifted.T.astype(jnp.float32), precision=exact_precision, preferred_element_type=jnp.float32)
    lag_sums = lax.map(one_lag, jnp.arange(M, dtype=jnp.int32))
    lag_sums = jnp.transpose(lag_sums, (1, 0, 2))
    counts = (NT - jnp.arange(M)).astype(jnp.float32)
    normed = lag_sums / counts[None, :, None]
    two_sided = jnp.concatenate([jnp.transpose(normed, (2, 1, 0))[:, :0:-1, :], normed], axis=1)

    def one_row(lag_index):
        window = lax.dynamic_slice(two_sided, (jnp.int32(0), (M - 1 - lag_index).astype(jnp.int32), jnp.int32(0)), (L, M, L))
        return window.reshape(L, M * L)
    covariance = lax.map(one_row, jnp.arange(M, dtype=jnp.int32)).reshape(M * L, M * L)
    factor = lower_factor(jnp.dot(start_block.T.astype(jnp.float32), start_block.astype(jnp.float32), precision=exact_precision, preferred_element_type=jnp.float32))
    current = jax.scipy.linalg.solve_triangular(factor, start_block.T, lower=True).T
    previous = jnp.zeros_like(current)
    upper = factor.T
    basis_list = [current]
    diagonal_list = []
    upper_list = [upper]
    for iteration in range(ITERS):
        work = jnp.dot(covariance.astype(jnp.float32), current.astype(jnp.float32), precision=exact_precision, preferred_element_type=jnp.float32)
        if iteration > 0:
            work = work - jnp.dot(previous.astype(jnp.float32), upper.T.astype(jnp.float32), precision=exact_precision, preferred_element_type=jnp.float32)
        diagonal = jnp.dot(current.T.astype(jnp.float32), work.astype(jnp.float32), precision=exact_precision, preferred_element_type=jnp.float32)
        work = work - jnp.dot(current.astype(jnp.float32), diagonal.astype(jnp.float32), precision=exact_precision, preferred_element_type=jnp.float32)
        factor = lower_factor(jnp.dot(work.T.astype(jnp.float32), work.astype(jnp.float32), precision=exact_precision, preferred_element_type=jnp.float32))
        upper = factor.T
        previous = current
        current = jax.scipy.linalg.solve_triangular(factor, work.T, lower=True).T
        basis_list.append(current)
        diagonal_list.append(diagonal)
        upper_list.append(upper)
    return (covariance, jnp.stack(basis_list), jnp.stack(diagonal_list), jnp.stack(upper_list))
```

```python
import jax
import jax.numpy as jnp
from jax import lax
from jax.experimental import pallas as pl
from jax.experimental.pallas import tpu as pltpu
from jax.sharding import PartitionSpec as P

M = 384
ITERS = 6
MESH = pl.DeviceIdType.MESH
EXACT = lax.Precision.HIGHEST
F32 = jnp.float32
BF16 = jnp.bfloat16
VMEM = pl.BlockSpec(memory_space=pltpu.VMEM)


def flip(index, mask):
    bit = 1
    while bit <= mask:
        if mask & bit:
            index = index + bit - 2 * bit * ((index // bit) % 2)
        bit *= 2
    return index


def round_up(value, unit):
    return -(-value // unit) * unit


class Plan:
    def __init__(self, channels, days, width, tm_size, panel_size):
        self.channels = channels
        self.days = days
        self.width = width
        self.tm_size = tm_size
        self.panel_size = panel_size
        self.lags = M // (tm_size * panel_size)
        self.phases = max(r for r in (1, 2, 3, 4) if self.lags % r == 0)
        self.groups = 8 if (8 * self.phases) % 16 == 0 else 16
        self.run = self.lags * panel_size
        self.pad = round_up(self.run + self.lags, self.groups * self.phases)
        self.reach = M + self.pad
        self.units = self.reach // self.phases
        self.steps = self.units // self.groups
        self.depth = days + 128
        self.heads = self.lags // self.phases
        self.rows = self.heads * channels
        self.lanes = 128 * ((self.phases * width + 127) // 128)
        self.columns = tm_size // 2


def series_kernel(size, s_ref, o_ref, held, send_sem, recv_sem):
    me = lax.axis_index("tm")
    days = s_ref.shape[1]
    barrier = pltpu.get_barrier_semaphore()
    for distance in range(1, size):
        pl.semaphore_signal(
            barrier, inc=1, device_id={"tm": (me + distance) % size}, device_id_type=MESH
        )
    pl.semaphore_wait(barrier, size - 1)
    copies = []
    for distance in range(1, size):
        copy = pltpu.make_async_remote_copy(
            src_ref=s_ref,
            dst_ref=held.at[distance],
            send_sem=send_sem.at[distance],
            recv_sem=recv_sem.at[distance],
            device_id={"tm": (me + distance) % size},
            device_id_type=MESH,
        )
        copy.start()
        copies.append(copy)
    o_ref[me] = s_ref[...]
    for distance, copy in enumerate(copies, 1):
        copy.wait_recv()
        o_ref[(me + size - distance) % size] = held[distance]
    for copy in copies:
        copy.wait_send()


def all_days(series, size):
    return pl.pallas_call(
        lambda *refs: series_kernel(size, *refs),
        out_shape=jax.ShapeDtypeStruct((size,) + series.shape, F32),
        in_specs=[VMEM],
        out_specs=VMEM,
        scratch_shapes=[
            pltpu.VMEM((size,) + series.shape, F32),
            pltpu.SemaphoreType.DMA((size,)),
            pltpu.SemaphoreType.DMA((size,)),
        ],
        compiler_params=pltpu.CompilerParams(collective_id=0, has_side_effects=True),
    )(series)


def covariance_kernel(plan, xh_ref, xl_ref, gh_ref, gl_ref, n_ref, near_ref, c_ref, wide, sem):
    channels, phases = plan.channels, plan.phases
    unit = plan.groups * channels
    together = max(g for g in (1, 2) if plan.steps % g == 0 and g * unit <= 768)

    def product(step, carry):
        pieces_h, pieces_l = [], []
        for g in range(together):
            start = pl.multiple_of((step * together + g) * plan.groups * phases, 16)
            pieces_h.append(gh_ref[pl.ds(start, plan.depth), :])
            pieces_l.append(gl_ref[pl.ds(start, plan.depth), :])
        high = jnp.concatenate(pieces_h, axis=1) if together > 1 else pieces_h[0]
        low = jnp.concatenate(pieces_l, axis=1) if together > 1 else pieces_l[0]
        total = jnp.dot(xh_ref[...], high, preferred_element_type=F32)
        total += jnp.dot(xh_ref[...], low, preferred_element_type=F32)
        total += jnp.dot(xl_ref[...], high, preferred_element_type=F32)
        at = pl.ds(pl.multiple_of(step * together * unit, 128), together * unit)
        counts = n_ref[:, at]
        for p in range(phases):
            rows = slice(p * channels, (p + 1) * channels)
            near_ref[rows, at] = total[rows] / counts[p : p + 1]
        return carry

    lax.fori_loop(0, plan.steps // together, product, 0)

    def weave(step, carry):
        block = near_ref[:, pl.ds(pl.multiple_of(step * unit, 128), unit)]
        pieces = [
            block[p * channels : (p + 1) * channels, g * channels : (g + 1) * channels]
            for g in range(plan.groups)
            for p in range(phases)
        ]
        at = pl.ds(pl.multiple_of(step * unit * phases, 128), unit * phases)
        wide[0, :, at] = jnp.concatenate(pieces, axis=1)
        return carry

    lax.fori_loop(0, plan.steps, weave, 0)

    total = plan.reach * channels
    core = lax.axis_index("tm") % 2
    jump = plan.run * channels
    if jump % 128:

        def choose(group, carry):
            rows = pl.ds(pl.multiple_of(group * 8, 8), 8)
            whole = wide[0, rows, :]
            back = pltpu.roll(whole, jump, 1)
            wide[0, rows, :] = jnp.where(core == 1, back, whole)
            return carry

        lax.fori_loop(0, channels // 8, choose, 0)
    slots = {}
    order = []
    for i in range(plan.lags):
        shift = ((plan.pad - i) * channels) % 128
        if shift not in slots:
            slots[shift] = len(slots)
    slots = {s: n for n, s in enumerate(sorted(slots))}
    copies = []
    for shift, slot in slots.items():
        if slot > 0:

            def turn(group, carry):
                rows = pl.ds(pl.multiple_of(group * 8, 8), 8)
                wide[slot, rows, :] = pltpu.roll(wide[0, rows, :], total - shift, 1)
                return carry

            lax.fori_loop(0, channels // 8, turn, 0)
        for i in range(plan.lags):
            first = (plan.pad - i) * channels
            if first % 128 != shift:
                continue
            start = first - shift
            if jump % 128 == 0:
                start = pl.multiple_of(start - jump * core, 128)
            copy = pltpu.make_async_copy(
                wide.at[slot, :, pl.ds(start, M * channels)],
                c_ref.at[pl.ds(i * channels, channels), :],
                sem.at[i],
            )
            copy.start()
            copies.append(copy)
    for copy in copies:
        copy.wait()


def split(array):
    high = lax.reduce_precision(array, 8, 7)
    return high.astype(BF16), (array - high).astype(BF16)


def covariance_rows(plan, days_by_device):
    channels, phases, days = plan.channels, plan.phases, plan.days
    size = plan.tm_size
    whole = jnp.transpose(days_by_device, (1, 0, 2)).reshape(channels, days)
    turned = jnp.transpose(days_by_device, (0, 2, 1)).reshape(days, channels)
    tm, panel = lax.axis_index("tm"), lax.axis_index("panel")
    base = -(tm // 2) * 2 * plan.run - panel * plan.lags - plan.pad
    stretch = plan.depth + plan.groups * phases * (plan.steps - 1)
    padded = jnp.pad(turned, ((M + plan.pad, plan.depth - days + M + plan.pad), (0, 0)))
    length = stretch + phases * (plan.groups - 1)
    near_days = lax.dynamic_slice(padded, (M + plan.pad + base, jnp.int32(0)), (length, channels))
    gathered = jnp.concatenate(
        [near_days[phases * g : phases * g + stretch] for g in range(plan.groups)], axis=1
    )
    shifted = jnp.concatenate(
        [jnp.pad(whole, ((0, 0), (p, plan.depth - days - p))) for p in range(phases)], axis=0
    )
    lag = base + jnp.arange(plan.units * channels) // channels * phases
    lag = lag[None, :] + jnp.arange(phases)[:, None]
    counts = (days - jnp.abs(lag)).astype(F32)
    shifts = len({((plan.pad - i) * channels) % 128 for i in range(plan.lags)} | {0})
    return pl.pallas_call(
        lambda *refs: covariance_kernel(plan, *refs),
        out_shape=(
            jax.ShapeDtypeStruct((phases * channels, plan.units * channels), F32),
            jax.ShapeDtypeStruct((plan.lags * channels, M * channels), F32),
        ),
        in_specs=[VMEM] * 5,
        out_specs=(VMEM, pl.BlockSpec(memory_space=pl.ANY)),
        scratch_shapes=[
            pltpu.VMEM((shifts, channels, plan.reach * channels), F32),
            pltpu.SemaphoreType.DMA((plan.lags,)),
        ],
        compiler_params=pltpu.CompilerParams(vmem_limit_bytes=60 * 1024 * 1024),
    )(*split(shifted), *split(gathered), counts)


def factor_and_inverse(gram, width):
    lanes = 2 * width
    row = lax.broadcasted_iota(jnp.int32, (width, lanes), 0)
    lane = lax.broadcasted_iota(jnp.int32, (width, lanes), 1)
    work = jnp.where(lane < width, gram, jnp.where(lane - width == row, 1.0, 0.0))
    for j in range(width):
        pivot_row = work[j : j + 1, :]
        scale = lax.rsqrt(jnp.broadcast_to(pivot_row[:, j : j + 1], (1, lanes)))
        pivot_row = pivot_row * scale
        column = jnp.broadcast_to(work[:, j : j + 1], (width, lanes)) * scale
        work = jnp.where(row > j, work - column * pivot_row, jnp.where(row == j, pivot_row, work))
    return jnp.where((lane < width) & (lane < row), 0.0, work)


def lanczos_kernel(
    plan,
    near_ref,
    x_ref,
    basis_ref,
    diag_ref,
    off_ref,
    lh,
    ll,
    zg,
    zh,
    zl,
    parts,
    q_s,
    z_s,
    v_s,
    guess,
    y_send,
    y_recv,
    g_held,
    g_got,
    p_send,
    p_recv,
    c_send,
    c_recv,
    g_send,
    g_recv,
    y_sems,
):
    channels, phases, width = plan.channels, plan.phases, plan.width
    heads, rows, lanes = plan.heads, plan.rows, plan.lanes
    panel_size, columns = plan.panel_size, plan.columns
    tm, panel = lax.axis_index("tm"), lax.axis_index("panel")
    core, k = tm % 2, tm // 2
    bits = columns.bit_length() - 1

    partners = [("tm", flip(tm, 1 << b)) for b in range(bits + 1)]
    partners += [("panel", flip(panel, d)) for d in range(1, panel_size)]
    barrier = pltpu.get_barrier_semaphore()
    for axis, other in partners:
        pl.semaphore_signal(barrier, inc=1, device_id={axis: other}, device_id_type=MESH)
    gram_partners = [("tm", flip(tm, 1 << b)) for b in range(bits + 1)]
    gram_partners += [
        ("panel", flip(panel, 1 << b)) for b in range(panel_size.bit_length() - 1)
    ]

    zero = jnp.zeros((rows, lanes), F32)
    q_s[...] = zero
    v_s[...] = zero
    z_s[...] = x_ref[...]
    guess[...] = jnp.zeros_like(guess)
    zg[0, k, panel] = x_ref[...]
    pl.semaphore_wait(barrier, len(partners))

    lane1 = lax.broadcasted_iota(jnp.int32, (width, 2 * width), 1)

    def spread(pair):
        low = jnp.where(lane1 < width, pair, 0.0)
        high = pltpu.roll(low, width, 1)
        none = jnp.zeros_like(low)
        out = []
        for p in range(lanes // width):
            here = low if p % 2 == 0 else high
            if p >= phases:
                here = none
            line = [here if t == p // 2 else none for t in range(lanes // (2 * width))]
            out.append(jnp.concatenate(line, axis=1) if len(line) > 1 else line[0])
        return jnp.concatenate(out, axis=0)

    def folded(square):
        even = odd = None
        for p in range(phases):
            block = square[p * width : (p + 1) * width, (p // 2) * 2 * width :][:, : 2 * width]
            if p % 2 == 0:
                even = block if even is None else even + block
            else:
                odd = block if odd is None else odd + block
        if odd is not None:
            even = even + pltpu.roll(odd, width, 1)
        return even

    def times(a, b):
        return jnp.dot(a, b, precision=EXACT, preferred_element_type=F32)

    def times_t(a, b):
        return lax.dot_general(
            a, b, (((1,), (1,)), ((), ())), precision=EXACT, preferred_element_type=F32
        )

    def t_times(a, b):
        return lax.dot_general(
            a, b, (((0,), (0,)), ((), ())), precision=EXACT, preferred_element_type=F32
        )

    def remote(src, dst, send, recv, axis, other):
        return pltpu.make_async_remote_copy(
            src_ref=src,
            dst_ref=dst,
            send_sem=send,
            recv_sem=recv,
            device_id={axis: other},
            device_id_type=MESH,
        )

    def panel_copy(par, d):
        slot = zg.at[par, k, panel]
        return remote(slot, slot, p_send.at[par, d], p_recv.at[par, d], "panel", flip(panel, d))

    def panel_arrival(par, d):
        slot = zg.at[par, k, flip(panel, d)]
        return remote(slot, slot, p_send.at[par, d], p_recv.at[par, d], "panel", flip(panel, d))

    orders = {}
    for d in range(panel_size):
        order = list(range(bits))
        orders[d] = order if d < panel_size // 2 else order[::-1]

    def column_copy(par, mask, d, bit):
        slot = zg.at[par, flip(k, mask), flip(panel, d)]
        n = (mask ^ (1 << bit)) * panel_size + d
        return remote(
            slot, slot, c_send.at[par, n], c_recv.at[par, n], "tm", flip(tm, 2 << bit)
        )

    def column_arrival(par, mask, d):
        order = orders[d]
        bit = [b for b in order if mask & (1 << b)][-1]
        slot = zg.at[par, flip(k, mask), flip(panel, d)]
        n = mask * panel_size + d
        return remote(
            slot, slot, c_send.at[par, n], c_recv.at[par, n], "tm", flip(tm, 2 << bit)
        )

    def last_stage(mask, d):
        return max([s for s, b in enumerate(orders[d]) if mask & (1 << b)], default=-1)

    def gram_copy(par, s):
        axis, other = gram_partners[s]
        return remote(
            g_held.at[par, s], g_got.at[par, s], g_send.at[par, s], g_recv.at[par, s], axis, other
        )

    def local_gram(par):
        q, z = q_s[...], z_s[...]
        first = folded(t_times(q, z))
        second = folded(t_times(z, z))
        g_held[par, 0] = jnp.where(lane1 < width, first, pltpu.roll(second, width, 1))
        gram_copy(par, 0).start()

    def gram_stage(par, s):
        copy = gram_copy(par, s)
        copy.wait_recv()
        g_held[par, s + 1] = g_held[par, s] + g_got[par, s]
        copy.wait_send()
        if s + 1 < len(gram_partners):
            gram_copy(par, s + 1).start()

    def small(par, j):
        both = g_held[par, len(gram_partners)]
        rest = jnp.where(lane1 < width, both, 0.0)
        square = t_times(rest, rest)[:width]
        gram = pltpu.roll(both, width, 1) - square
        work = factor_and_inverse(gram, width)
        diag = rest + guess[...]
        diag_ref[j] = diag[:, :width]
        off_ref[j] = work[:, :width]
        spread_rest = spread(rest)
        spread_r = spread(work)
        spread_l = spread(pltpu.roll(work, width, 1))
        q = q_s[...]
        after = z_s[...] - times(q, spread_rest)
        following = times_t(after, spread_l)
        for p in range(phases):
            block = following[:, (p // 2) * 2 * width :][:, : 2 * width]
            if p % 2:
                block = pltpu.roll(block, width, 1)
            for h in range(heads):
                basis_ref[j, pl.ds((h * phases + p) * channels, channels), :] = block[
                    h * channels : (h + 1) * channels, :width
                ]
        return diag, spread_rest, spread_r, spread_l, following

    def build(own):
        total = plan.units * channels
        back = plan.run // phases * channels
        stride = 2 * back
        for p in range(phases):

            def chunk(c, carry):
                at = pl.multiple_of(p * channels + c * 16, 16)
                part = near_ref[pl.ds(at, 16), :]
                if not own:
                    part = jnp.where(
                        core == 1, pltpu.roll(part, total - back, 1), pltpu.roll(part, back, 1)
                    )
                for i in range(1 - phases, plan.lags):
                    if (plan.pad - i - p) % phases:
                        continue
                    u0 = (plan.pad - i - p) // phases
                    turned = pltpu.roll(part, total - u0 * channels, 1)
                    pieces = [turned[:, n * stride : n * stride + back] for n in range(columns)]
                    line = jnp.concatenate(pieces, axis=1)
                    high = line.astype(BF16)
                    low = (line - high.astype(F32)).astype(BF16)
                    to = pl.ds(pl.multiple_of((i + phases - 1) * channels + c * 16, 16), 16)
                    lh[int(own), to, :] = high
                    ll[int(own), to, :] = low
                return carry

            lax.fori_loop(0, channels // 16, chunk, 0)

    def product(which):
        high, low = zh[...], zl[...]
        parts[...] = jnp.dot(lh[which], high, preferred_element_type=F32)
        parts[...] += jnp.dot(lh[which], low, preferred_element_type=F32)
        parts[...] += jnp.dot(ll[which], high, preferred_element_type=F32)
        lane = lax.broadcasted_iota(jnp.int32, (channels, lanes), 1)
        out = []
        for h in range(heads):
            total = None
            for delta in range(1 - phases, phases):
                i = h * phases + delta + phases - 1
                term = parts[i * channels : (i + 1) * channels, :]
                if delta:
                    term = pltpu.roll(term, (delta * width) % lanes, 1)
                    if delta > 0:
                        keep = lane >= delta * width
                    else:
                        keep = lane < (phases + delta) * width
                    term = jnp.where(keep, term, 0.0)
                total = term if total is None else total + term
            out.append(total)
        whole = jnp.concatenate(out, axis=0) if heads > 1 else out[0]
        if phases * width < lanes:
            whole = jnp.where(
                lax.broadcasted_iota(jnp.int32, whole.shape, 1) < phases * width, whole, 0.0
            )
        return whole

    def iteration(j, carry):
        par = j % 2
        sends = []
        for d in range(1, panel_size):
            copy = panel_copy(par, d)
            copy.start()
            sends.append(copy)
        for bit in orders[0]:
            copy = column_copy(par, 0, 0, bit)
            copy.start()
            sends.append(copy)
        local_gram(par)
        stages = list(range(len(gram_partners)))

        def next_stage():
            if stages:
                gram_stage(par, stages.pop(0))

        for d in range(1, panel_size):
            panel_arrival(par, d).wait_recv()
            for bit in orders[d]:
                copy = column_copy(par, 0, d, bit)
                copy.start()
                sends.append(copy)
            next_stage()
        waited = set()
        for s in range(bits - 1):
            for d in range(panel_size):
                for mask in range(1, columns):
                    if last_stage(mask, d) != s:
                        continue
                    column_arrival(par, mask, d).wait_recv()
                    waited.add((mask, d))
                    for bit in orders[d][s + 1 :]:
                        copy = column_copy(par, mask, d, bit)
                        copy.start()
                        sends.append(copy)
                    next_stage()
        while stages:
            next_stage()
        diag, spread_rest, spread_r, spread_l, following = small(par, j)
        v_part = times(v_s[...], spread_rest)
        q_r = times_t(q_s[...], spread_r) + times(following, spread(diag))
        guess[...] = diag

        @pl.when(j == 0)
        def _():
            build(False)
            build(True)

        for mask in range(1, columns):
            for d in range(panel_size):
                if (mask, d) not in waited:
                    column_arrival(par, mask, d).wait_recv()
        for n in range(columns):
            for d in range(panel_size):
                block = zg[par, n, d]
                high = block.astype(BF16)
                at = pl.ds((n * panel_size + d) * rows, rows)
                zh[at, :] = high
                zl[at, :] = (block - high.astype(F32)).astype(BF16)
        y_send[par] = product(0)
        to_other = remote(
            y_send.at[par], y_recv.at[par], y_sems.at[par, 0], y_sems.at[par, 1], "tm", flip(tm, 1)
        )
        to_other.start()
        mine = product(1)
        to_other.wait_recv()
        y = mine + y_recv[par]
        v = times_t(y - v_part, spread_l)
        z = v - q_r
        v_s[...] = v
        z_s[...] = z
        q_s[...] = following
        zg[1 - par, k, panel] = z
        for copy in sends:
            copy.wait_send()
        to_other.wait_send()
        return carry

    lax.fori_loop(0, ITERS, iteration, 0)
    par = ITERS % 2
    local_gram(par)
    for s in range(len(gram_partners)):
        gram_stage(par, s)
    small(par, ITERS)


def lanczos(plan, near, packed):
    channels, phases, width = plan.channels, plan.phases, plan.width
    rows, lanes = plan.rows, plan.lanes
    blocks = plan.columns * plan.panel_size
    groups = (plan.lags + phases - 1) * channels
    stages = (plan.tm_size * plan.panel_size).bit_length() - 1
    block = (rows, lanes)
    pair = (width, 2 * width)
    dma = pltpu.SemaphoreType.DMA
    return pl.pallas_call(
        lambda *refs: lanczos_kernel(plan, *refs),
        out_shape=(
            jax.ShapeDtypeStruct((ITERS + 1, plan.lags * channels, width), F32),
            jax.ShapeDtypeStruct((ITERS + 1, width, width), F32),
            jax.ShapeDtypeStruct((ITERS + 1, width, width), F32),
        ),
        in_specs=[VMEM] * 2,
        out_specs=(VMEM,) * 3,
        scratch_shapes=[
            pltpu.VMEM((2, groups, blocks * rows), BF16),
            pltpu.VMEM((2, groups, blocks * rows), BF16),
            pltpu.VMEM((2, plan.columns, plan.panel_size) + block, F32),
            pltpu.VMEM((blocks * rows, lanes), BF16),
            pltpu.VMEM((blocks * rows, lanes), BF16),
            pltpu.VMEM((groups, lanes), F32),
            pltpu.VMEM(block, F32),
            pltpu.VMEM(block, F32),
            pltpu.VMEM(block, F32),
            pltpu.VMEM(pair, F32),
            pltpu.VMEM((2,) + block, F32),
            pltpu.VMEM((2,) + block, F32),
            pltpu.VMEM((2, stages + 1) + pair, F32),
            pltpu.VMEM((2, stages) + pair, F32),
            dma((2, plan.panel_size)),
            dma((2, plan.panel_size)),
            dma((2, blocks)),
            dma((2, blocks * max(1, plan.columns.bit_length()))),
            dma((2, stages)),
            dma((2, stages)),
            dma((2, 2)),
        ],
        compiler_params=pltpu.CompilerParams(
            collective_id=1, has_side_effects=True, vmem_limit_bytes=60 * 1024 * 1024
        ),
    )(near, packed)


def local(series, start_block):
    channels, day_count = series.shape
    tm_size = lax.axis_size("tm")
    panel_size = lax.axis_size("panel")
    width = start_block.shape[1]
    plan = Plan(channels, day_count * tm_size, width, tm_size, panel_size)
    near, covariance = covariance_rows(plan, all_days(series, tm_size))
    packed = start_block.reshape(plan.heads, plan.phases, channels, width)
    packed = jnp.transpose(packed, (0, 2, 1, 3)).reshape(plan.rows, plan.phases * width)
    packed = jnp.pad(packed, ((0, 0), (0, plan.lanes - plan.phases * width)))
    basis, diag, off = lanczos(plan, near, packed)
    return covariance, basis, diag[1:], off


def solution(mesh):
    placed = (P(None, "tm"), P(("tm", "panel"), None))
    return jax.shard_map(
        local,
        mesh=mesh,
        in_specs=placed,
        out_specs=(P(("tm", "panel"), None), P(None, ("tm", "panel"), None), P(), P()),
        check_vma=False,
    )
```

```python
import jax
import jax.numpy as jnp
from jax import lax
from jax.experimental import pallas as pl
from jax.experimental.pallas import tpu as pltpu
from jax.sharding import PartitionSpec as P

M = 384
ITERS = 6
MESH = pl.DeviceIdType.MESH
EXACT = lax.Precision.HIGHEST
F32 = jnp.float32
BF16 = jnp.bfloat16
VMEM = pl.BlockSpec(memory_space=pltpu.VMEM)


def flip(index, mask):
    bit = 1
    while bit <= mask:
        if mask & bit:
            index = index + bit - 2 * bit * ((index // bit) % 2)
        bit *= 2
    return index


def round_up(value, unit):
    return -(-value // unit) * unit


class Plan:
    def __init__(self, channels, days, width, tm_size, panel_size):
        self.channels = channels
        self.days = days
        self.width = width
        self.tm_size = tm_size
        self.panel_size = panel_size
        self.lags = M // (tm_size * panel_size)
        self.phases = max(r for r in (1, 2, 3, 4) if self.lags % r == 0)
        self.groups = 8 if (8 * self.phases) % 16 == 0 else 16
        self.run = self.lags * panel_size
        self.pad = round_up(self.run + 2 * self.lags, self.groups * self.phases)
        self.reach = round_up(M + self.pad + self.lags, (16 // self.groups) * 32)
        self.reach = round_up(self.reach, self.groups * self.phases)
        self.units = self.reach // self.phases
        self.steps = self.units // self.groups
        self.depth = days + 128
        self.heads = self.lags // self.phases
        self.rows = self.heads * channels
        self.lanes = 128 * ((self.phases * width + 127) // 128)
        self.columns = tm_size // 2
        self.halves = panel_size // 2

    def offset(self, tm, panel):
        return (tm // 2) * 2 * self.run + panel * self.lags + self.pad


def series_kernel(size, s_ref, o_ref, held, send_sem, recv_sem):
    me = lax.axis_index("tm")
    days = s_ref.shape[1]
    barrier = pltpu.get_barrier_semaphore()
    for distance in range(1, size):
        pl.semaphore_signal(
            barrier, inc=1, device_id={"tm": (me + distance) % size}, device_id_type=MESH
        )
    pl.semaphore_wait(barrier, size - 1)
    copies = []
    for distance in range(1, size):
        copy = pltpu.make_async_remote_copy(
            src_ref=s_ref,
            dst_ref=held.at[distance],
            send_sem=send_sem.at[distance],
            recv_sem=recv_sem.at[distance],
            device_id={"tm": (me + distance) % size},
            device_id_type=MESH,
        )
        copy.start()
        copies.append(copy)
    o_ref[me] = s_ref[...]
    for distance, copy in enumerate(copies, 1):
        copy.wait_recv()
        o_ref[(me + size - distance) % size] = held[distance]
    for copy in copies:
        copy.wait_send()


def all_days(series, size):
    return pl.pallas_call(
        lambda *refs: series_kernel(size, *refs),
        out_shape=jax.ShapeDtypeStruct((size,) + series.shape, F32),
        in_specs=[VMEM],
        out_specs=VMEM,
        scratch_shapes=[
            pltpu.VMEM((size,) + series.shape, F32),
            pltpu.SemaphoreType.DMA((size,)),
            pltpu.SemaphoreType.DMA((size,)),
        ],
        compiler_params=pltpu.CompilerParams(collective_id=0, has_side_effects=True),
    )(series)


def covariance_kernel(
    plan, d_ref, n_ref, near_ref, c_ref, xh_ref, xl_ref, gh_ref, gl_ref, moved, wide, sem
):
    channels, phases = plan.channels, plan.phases
    unit = plan.groups * channels
    tm, panel = lax.axis_index("tm"), lax.axis_index("panel")
    length = moved.shape[1]
    for n in range(d_ref.shape[0]):
        moved[:, n * d_ref.shape[2] : (n + 1) * d_ref.shape[2]] = d_ref[n]
    moved[:, plan.days :] = jnp.zeros((channels, length - plan.days), F32)
    for p in range(phases):
        rows = slice(p * channels, (p + 1) * channels)
        shifted = moved[:, : plan.depth]
        if p:
            shifted = pltpu.roll(shifted, p, 1)
        high = shifted.astype(BF16)
        xh_ref[rows, :] = high
        xl_ref[rows, :] = (shifted - high.astype(F32)).astype(BF16)
    moved[...] = pltpu.roll(moved[...], plan.offset(tm, panel), 1)

    def transpose(step, carry):
        at = pl.multiple_of(step * 128, 128)
        window = moved[:, pl.ds(at, 256)]
        stack = [window[:, phases * g : phases * g + 128] for g in range(plan.groups)]
        block = jnp.concatenate(stack, axis=0).T
        high = block.astype(BF16)
        gh_ref[pl.ds(at, 128), :] = high
        gl_ref[pl.ds(at, 128), :] = (block - high.astype(F32)).astype(BF16)
        return carry

    lax.fori_loop(0, gh_ref.shape[0] // 128, transpose, 0)
    together = max(g for g in (1, 2) if plan.steps % g == 0 and g * unit <= 768)

    def product(step, carry):
        pieces_h, pieces_l = [], []
        for g in range(together):
            start = pl.multiple_of((step * together + g) * plan.groups * phases, 16)
            pieces_h.append(gh_ref[pl.ds(start, plan.depth), :])
            pieces_l.append(gl_ref[pl.ds(start, plan.depth), :])
        high = jnp.concatenate(pieces_h, axis=1) if together > 1 else pieces_h[0]
        low = jnp.concatenate(pieces_l, axis=1) if together > 1 else pieces_l[0]
        total = jnp.dot(xh_ref[...], high, preferred_element_type=F32)
        total += jnp.dot(xh_ref[...], low, preferred_element_type=F32)
        total += jnp.dot(xl_ref[...], high, preferred_element_type=F32)
        at = pl.ds(pl.multiple_of(step * together * unit, 128), together * unit)
        counts = n_ref[:, at]
        for p in range(phases):
            rows = slice(p * channels, (p + 1) * channels)
            near_ref[rows, at] = total[rows] / counts[p : p + 1]
        return carry

    lax.fori_loop(0, plan.steps // together, product, 0)

    def weave(step, carry):
        block = near_ref[:, pl.ds(pl.multiple_of(step * unit, 128), unit)]
        pieces = [
            block[p * channels : (p + 1) * channels, g * channels : (g + 1) * channels]
            for g in range(plan.groups)
            for p in range(phases)
        ]
        at = pl.ds(pl.multiple_of(step * unit * phases, 128), unit * phases)
        wide[0, :, at] = jnp.concatenate(pieces, axis=1)
        return carry

    lax.fori_loop(0, plan.steps, weave, 0)

    total = plan.reach * channels
    core = lax.axis_index("tm") % 2
    jump = plan.run * channels
    if jump % 128:

        def choose(group, carry):
            rows = pl.ds(pl.multiple_of(group * 8, 8), 8)
            whole = wide[0, rows, :]
            back = pltpu.roll(whole, jump, 1)
            wide[0, rows, :] = jnp.where(core == 1, back, whole)
            return carry

        lax.fori_loop(0, channels // 8, choose, 0)
    slots = {}
    order = []
    for i in range(plan.lags):
        shift = ((plan.pad - i) * channels) % 128
        if shift not in slots:
            slots[shift] = len(slots)
    slots = {s: n for n, s in enumerate(sorted(slots))}
    copies = []
    for shift, slot in slots.items():
        if slot > 0:

            def turn(group, carry):
                rows = pl.ds(pl.multiple_of(group * 8, 8), 8)
                wide[slot, rows, :] = pltpu.roll(wide[0, rows, :], total - shift, 1)
                return carry

            lax.fori_loop(0, channels // 8, turn, 0)
        for i in range(plan.lags):
            first = (plan.pad - i) * channels
            if first % 128 != shift:
                continue
            start = first - shift
            if jump % 128 == 0:
                start = pl.multiple_of(start - jump * core, 128)
            copy = pltpu.make_async_copy(
                wide.at[slot, :, pl.ds(start, M * channels)],
                c_ref.at[pl.ds(i * channels, channels), :],
                sem.at[i],
            )
            copy.start()
            copies.append(copy)
    for copy in copies:
        copy.wait()


def covariance_rows(plan, days_by_device):
    channels, phases, days = plan.channels, plan.phases, plan.days
    base = -plan.offset(lax.axis_index("tm"), lax.axis_index("panel"))
    stretch = round_up(plan.depth + plan.groups * phases * (plan.steps - 1), 128)
    lag = base + jnp.arange(plan.units * channels) // channels * phases
    lag = lag[None, :] + jnp.arange(phases)[:, None]
    counts = (days - jnp.abs(lag)).astype(F32)
    shifts = len({((plan.pad - i) * channels) % 128 for i in range(plan.lags)} | {0})
    return pl.pallas_call(
        lambda *refs: covariance_kernel(plan, *refs),
        out_shape=(
            jax.ShapeDtypeStruct((phases * channels, plan.units * channels), F32),
            jax.ShapeDtypeStruct((plan.lags * channels, M * channels), F32),
        ),
        in_specs=[VMEM] * 2,
        out_specs=(VMEM, pl.BlockSpec(memory_space=pl.ANY)),
        scratch_shapes=[
            pltpu.VMEM((phases * channels, plan.depth), BF16),
            pltpu.VMEM((phases * channels, plan.depth), BF16),
            pltpu.VMEM((stretch, plan.groups * channels), BF16),
            pltpu.VMEM((stretch, plan.groups * channels), BF16),
            pltpu.VMEM((channels, max(stretch + 128, days + plan.reach)), F32),
            pltpu.VMEM((shifts, channels, plan.reach * channels), F32),
            pltpu.SemaphoreType.DMA((plan.lags,)),
        ],
        compiler_params=pltpu.CompilerParams(vmem_limit_bytes=60 * 1024 * 1024),
    )(days_by_device, counts)


def factor_and_inverse(gram, width):
    lanes = 2 * width
    row = lax.broadcasted_iota(jnp.int32, (width, lanes), 0)
    lane = lax.broadcasted_iota(jnp.int32, (width, lanes), 1)
    work = jnp.where(lane < width, gram, jnp.where(lane - width == row, 1.0, 0.0))
    for j in range(width):
        pivot_row = work[j : j + 1, :]
        scale = lax.rsqrt(jnp.broadcast_to(pivot_row[:, j : j + 1], (1, lanes)))
        pivot_row = pivot_row * scale
        column = jnp.broadcast_to(work[:, j : j + 1], (width, lanes)) * scale
        work = jnp.where(row > j, work - column * pivot_row, jnp.where(row == j, pivot_row, work))
    return jnp.where((lane < width) & (lane < row), 0.0, work)


def lanczos_kernel(
    plan,
    near_ref,
    x_ref,
    basis_ref,
    diag_ref,
    off_ref,
    left,
    zg,
    right,
    parts,
    q_s,
    z_s,
    v_s,
    guess,
    y_send,
    y_recv,
    g_held,
    g_got,
    p_send,
    p_recv,
    c_send,
    c_recv,
    g_send,
    g_recv,
    y_sems,
):
    channels, phases, width = plan.channels, plan.phases, plan.width
    heads, rows, lanes = plan.heads, plan.rows, plan.lanes
    panel_size, columns, halves = plan.panel_size, plan.columns, plan.halves
    tm, panel = lax.axis_index("tm"), lax.axis_index("panel")
    core, k = tm % 2, tm // 2
    side, half = panel % 2, panel // 2
    bits = columns.bit_length() - 1

    gram_stages = [[("tm", flip(tm, 1))]]
    gram_stages.append([("tm", flip(tm, 2 * m)) for m in range(1, columns)])
    gram_stages.append([("panel", flip(panel, d)) for d in range(1, panel_size)])
    partners = [partner for stage in gram_stages for partner in stage]
    barrier = pltpu.get_barrier_semaphore()
    for axis, other in partners:
        pl.semaphore_signal(barrier, inc=1, device_id={axis: other}, device_id_type=MESH)

    zero = jnp.zeros((rows, lanes), F32)
    q_s[...] = zero
    v_s[...] = zero
    z_s[...] = x_ref[...]
    guess[...] = jnp.zeros_like(guess)
    zg[0, k, half] = x_ref[...]
    pl.semaphore_wait(barrier, len(partners))

    lane1 = lax.broadcasted_iota(jnp.int32, (width, 2 * width), 1)

    def spread(pair):
        low = jnp.where(lane1 < width, pair, 0.0)
        high = pltpu.roll(low, width, 1)
        none = jnp.zeros_like(low)
        out = []
        for p in range(lanes // width):
            here = low if p % 2 == 0 else high
            if p >= phases:
                here = none
            line = [here if t == p // 2 else none for t in range(lanes // (2 * width))]
            out.append(jnp.concatenate(line, axis=1) if len(line) > 1 else line[0])
        return jnp.concatenate(out, axis=0)

    def folded(square):
        even = odd = None
        for p in range(phases):
            block = square[p * width : (p + 1) * width, (p // 2) * 2 * width :][:, : 2 * width]
            if p % 2 == 0:
                even = block if even is None else even + block
            else:
                odd = block if odd is None else odd + block
        if odd is not None:
            even = even + pltpu.roll(odd, width, 1)
        return even

    def times(a, b):
        return jnp.dot(a, b, precision=EXACT, preferred_element_type=F32)

    def times_t(a, b):
        return lax.dot_general(
            a, b, (((1,), (1,)), ((), ())), precision=EXACT, preferred_element_type=F32
        )

    def t_times(a, b):
        return lax.dot_general(
            a, b, (((0,), (0,)), ((), ())), precision=EXACT, preferred_element_type=F32
        )

    def remote(src, dst, send, recv, axis, other):
        return pltpu.make_async_remote_copy(
            src_ref=src,
            dst_ref=dst,
            send_sem=send,
            recv_sem=recv,
            device_id={axis: other},
            device_id_type=MESH,
        )

    def panel_copy(par, d):
        slot = zg.at[par, k, half]
        other = flip(panel, 2 * d)
        return remote(slot, slot, p_send.at[par, d], p_recv.at[par, d], "panel", other)

    def panel_arrival(par, d):
        slot = zg.at[par, k, flip(half, d)]
        other = flip(panel, 2 * d)
        return remote(slot, slot, p_send.at[par, d], p_recv.at[par, d], "panel", other)

    orders = {}
    for d in range(halves):
        order = list(range(bits))
        orders[d] = order if d < (halves + 1) // 2 else order[::-1]

    def column_copy(par, mask, d, bit):
        slot = zg.at[par, flip(k, mask), flip(half, d)]
        n = (mask ^ (1 << bit)) * halves + d
        return remote(
            slot, slot, c_send.at[par, n], c_recv.at[par, n], "tm", flip(tm, 2 << bit)
        )

    def column_arrival(par, mask, d):
        order = orders[d]
        bit = [b for b in order if mask & (1 << b)][-1]
        slot = zg.at[par, flip(k, mask), flip(half, d)]
        n = mask * halves + d
        return remote(
            slot, slot, c_send.at[par, n], c_recv.at[par, n], "tm", flip(tm, 2 << bit)
        )

    def last_stage(mask, d):
        return max([s for s, b in enumerate(orders[d]) if mask & (1 << b)], default=-1)

    def gram_copies(par, s):
        first = sum(len(stage) for stage in gram_stages[:s])
        return [
            remote(
                g_held.at[par, s],
                g_got.at[par, first + n],
                g_send.at[par, first + n],
                g_recv.at[par, first + n],
                axis,
                other,
            )
            for n, (axis, other) in enumerate(gram_stages[s])
        ]

    def gram_send(par, s):
        copies = gram_copies(par, s)
        for copy in copies:
            copy.start()
        return copies

    def local_gram(par):
        z = z_s[...]
        both = t_times(jnp.concatenate([q_s[...], z], axis=1), z)
        first = folded(both[:lanes])
        second = folded(both[lanes:])
        g_held[par, 0] = jnp.where(lane1 < width, first, pltpu.roll(second, width, 1))
        return gram_send(par, 0)

    def gram_stage(par, s, copies):
        first = sum(len(stage) for stage in gram_stages[:s])
        terms = [g_held[par, s]]
        for n, copy in enumerate(copies):
            copy.wait_recv()
            terms.append(g_got[par, first + n])
        while len(terms) > 1:
            terms = [terms[n] + terms[n + 1] for n in range(0, len(terms), 2)]
        g_held[par, s + 1] = terms[0]
        return gram_send(par, s + 1) if s + 1 < len(gram_stages) else []

    def small(par, j):
        both = g_held[par, len(gram_stages)]
        rest = jnp.where(lane1 < width, both, 0.0)
        square = t_times(rest, rest)[:width]
        gram = pltpu.roll(both, width, 1) - square
        work = factor_and_inverse(gram, width)
        diag = rest + guess[...]
        diag_ref[j] = diag[:, :width]
        off_ref[j] = work[:, :width]
        spread_rest = spread(rest)
        spread_r = spread(work)
        spread_l = spread(pltpu.roll(work, width, 1))
        products = times(jnp.concatenate([q_s[...], v_s[...]], axis=0), spread_rest)
        after = z_s[...] - products[:rows]
        following = times_t(after, spread_l)
        for p in range(phases):
            block = following[:, (p // 2) * 2 * width :][:, : 2 * width]
            if p % 2:
                block = pltpu.roll(block, width, 1)
            for h in range(heads):
                basis_ref[j, pl.ds((h * phases + p) * channels, channels), :] = block[
                    h * channels : (h + 1) * channels, :width
                ]
        return diag, products[rows:], spread_r, spread_l, following

    def build(same_core, same_side):
        total = plan.units * channels
        ahead = side if same_side else 3 * side - 1
        ahead = ahead * heads
        if not same_core:
            ahead = ahead + (2 * core - 1) * (plan.run // phases)
        turn = (total - ahead * channels) % total
        variant = 2 * int(same_core) + int(same_side)
        stride = 2 * plan.run // phases * channels
        piece = heads * channels
        for p in range(phases):

            def chunk(c, carry):
                at = pl.multiple_of(p * channels + c * 16, 16)
                part = pltpu.roll(near_ref[pl.ds(at, 16), :], turn, 1)
                for i in range(1 - phases, plan.lags):
                    if (plan.pad - i - p) % phases:
                        continue
                    u0 = (plan.pad - i - p) // phases
                    to = pl.ds(pl.multiple_of((i + phases - 1) * channels + c * 16, 16), 16)
                    for h in range(halves):
                        pieces = []
                        for n in range(columns):
                            start = u0 * channels + n * stride + 2 * h * piece
                            pieces.append(part[:, start : start + piece])
                        line = jnp.concatenate(pieces, axis=1)
                        high = line.astype(BF16)
                        low = (line - high.astype(F32)).astype(BF16)
                        depth = line.shape[1]
                        left[variant, h, to, :depth] = high
                        left[variant, h, to, depth : 2 * depth] = high
                        left[variant, h, to, 2 * depth :] = low
                return carry

            lax.fori_loop(0, channels // 16, chunk, 0)

    def add_product(variant, which, first):
        total = jnp.dot(left[variant, which], right[which], preferred_element_type=F32)
        parts[variant] = total if first else parts[variant] + total

    def combined(variant):
        lane = lax.broadcasted_iota(jnp.int32, (channels, lanes), 1)
        out = []
        for h in range(heads):
            total = None
            for delta in range(1 - phases, phases):
                i = h * phases + delta + phases - 1
                term = parts[variant, i * channels : (i + 1) * channels, :]
                if delta:
                    term = pltpu.roll(term, (delta * width) % lanes, 1)
                    if delta > 0:
                        keep = lane >= delta * width
                    else:
                        keep = lane < (phases + delta) * width
                    term = jnp.where(keep, term, 0.0)
                total = term if total is None else total + term
            out.append(total)
        whole = jnp.concatenate(out, axis=0) if heads > 1 else out[0]
        if phases * width < lanes:
            whole = jnp.where(
                lax.broadcasted_iota(jnp.int32, whole.shape, 1) < phases * width, whole, 0.0
            )
        return whole

    def take_in(par, mask, d):
        column = flip(k, mask)
        block = zg[par, column, flip(half, d)]
        high = block.astype(BF16)
        low = (block - high.astype(F32)).astype(BF16)
        for n, term in enumerate((high, low, high)):
            to = pl.ds(pl.multiple_of((n * columns + column) * rows, 16), rows)
            right[flip(half, d), to, :] = term

    events = [(2.0, "gram", 0), (6.5, "gram", 1), (13.0, "gram", 2), (13.5, "small", 0)]
    events.append((9.5, "products", 0))
    for d in range(halves):
        if d:
            events.append((7.0 * d, "panel", d))
        for mask in range(1, columns):
            if last_stage(mask, d) < bits - 1:
                hops = bin(mask).count("1")
                events.append((7.0 * d + 4.5 * hops, "column", (mask, d)))
    events.sort(key=lambda event: event[0])

    def iteration(j, carry):
        par = j % 2
        sends = []

        def forward(mask, d):
            for bit in orders[d][last_stage(mask, d) + 1 :]:
                copy = column_copy(par, mask, d, bit)
                copy.start()
                sends.append(copy)

        def arrive(mask, d):
            arrival = column_arrival(par, mask, d) if mask else panel_arrival(par, d)
            arrival.wait_recv()
            forward(mask, d)
            take_in(par, mask, d)
            arrived.add((mask, d))

        def arrive_half(d):
            for mask in range(columns):
                if (mask, d) not in arrived:
                    arrive(mask, d)

        for d in range(1, halves):
            copy = panel_copy(par, d)
            copy.start()
            sends.append(copy)
        forward(0, 0)

        @pl.when(j == 0)
        def _():
            for same_core in (False, True):
                for same_side in (False, True):
                    build(same_core, same_side)

        gram = local_gram(par)
        sends += gram
        take_in(par, 0, 0)
        arrived = {(0, 0)}
        for _, kind, what in events:
            if kind == "gram":
                gram = gram_stage(par, what, gram)
                sends += gram
            elif kind == "small":
                diag, v_part, spread_r, spread_l, following = small(par, j)
                q_r = times_t(q_s[...], spread_r) + times(following, spread(diag))
            elif kind == "products":
                for d in range(halves - 1):
                    arrive_half(d)
                    for variant in range(4):
                        add_product(variant, flip(half, d), d == 0)
            elif kind == "panel":
                arrive(0, what)
            else:
                arrive(*what)
        guess[...] = diag
        last = halves - 1
        arrive_half(last)
        across = {}

        def to_core(other_side):
            variant = 1 - other_side
            add_product(variant, flip(half, last), last == 0)
            y_send[par, other_side] = combined(variant)
            copy = remote(
                y_send.at[par, other_side],
                y_recv.at[par, other_side],
                y_sems.at[par, other_side],
                y_sems.at[par, 2 + other_side],
                "tm",
                flip(tm, 1),
            )
            copy.start()
            across[other_side] = copy

        to_core(1)
        add_product(2, flip(half, last), last == 0)
        near_side = combined(2)
        across[1].wait_recv()
        y_send[par, 2] = near_side + y_recv[par, 1]
        over = remote(
            y_send.at[par, 2],
            y_recv.at[par, 2],
            y_sems.at[par, 4],
            y_sems.at[par, 5],
            "panel",
            flip(panel, 1),
        )
        over.start()
        to_core(0)
        add_product(3, flip(half, last), last == 0)
        mine = combined(3) - v_part
        across[0].wait_recv()
        mine = mine + y_recv[par, 0]
        over.wait_recv()
        v = times_t(mine + y_recv[par, 2], spread_l)
        z = v - q_r
        v_s[...] = v
        z_s[...] = z
        q_s[...] = following
        zg[1 - par, k, half] = z
        for copy in sends + [across[0], across[1], over]:
            copy.wait_send()
        return carry

    lax.fori_loop(0, ITERS, iteration, 0)
    par = ITERS % 2
    gram = local_gram(par)
    sends = list(gram)
    for s in range(len(gram_stages)):
        gram = gram_stage(par, s, gram)
        sends += gram
    small(par, ITERS)
    for copy in sends:
        copy.wait_send()


def lanczos(plan, near, packed):
    channels, phases, width = plan.channels, plan.phases, plan.width
    rows, lanes = plan.rows, plan.lanes
    blocks = plan.columns * plan.halves
    groups = (plan.lags + phases - 1) * channels
    others = plan.columns + plan.panel_size - 1
    block = (rows, lanes)
    pair = (width, 2 * width)
    dma = pltpu.SemaphoreType.DMA
    return pl.pallas_call(
        lambda *refs: lanczos_kernel(plan, *refs),
        out_shape=(
            jax.ShapeDtypeStruct((ITERS + 1, plan.lags * channels, width), F32),
            jax.ShapeDtypeStruct((ITERS + 1, width, width), F32),
            jax.ShapeDtypeStruct((ITERS + 1, width, width), F32),
        ),
        in_specs=[VMEM] * 2,
        out_specs=(VMEM,) * 3,
        scratch_shapes=[
            pltpu.VMEM((4, plan.halves, groups, 3 * plan.columns * rows), BF16),
            pltpu.VMEM((2, plan.columns, plan.halves) + block, F32),
            pltpu.VMEM((plan.halves, 3 * plan.columns * rows, lanes), BF16),
            pltpu.VMEM((4, groups, lanes), F32),
            pltpu.VMEM(block, F32),
            pltpu.VMEM(block, F32),
            pltpu.VMEM(block, F32),
            pltpu.VMEM(pair, F32),
            pltpu.VMEM((2, 3) + block, F32),
            pltpu.VMEM((2, 3) + block, F32),
            pltpu.VMEM((2, 4) + pair, F32),
            pltpu.VMEM((2, others) + pair, F32),
            dma((2, plan.halves)),
            dma((2, plan.halves)),
            dma((2, blocks)),
            dma((2, blocks)),
            dma((2, others)),
            dma((2, others)),
            dma((2, 6)),
        ],
        compiler_params=pltpu.CompilerParams(
            collective_id=1, has_side_effects=True, vmem_limit_bytes=60 * 1024 * 1024
        ),
    )(near, packed)


def local(series, start_block):
    channels, day_count = series.shape
    tm_size = lax.axis_size("tm")
    panel_size = lax.axis_size("panel")
    width = start_block.shape[1]
    plan = Plan(channels, day_count * tm_size, width, tm_size, panel_size)
    near, covariance = covariance_rows(plan, all_days(series, tm_size))
    packed = start_block.reshape(plan.heads, plan.phases, channels, width)
    packed = jnp.transpose(packed, (0, 2, 1, 3)).reshape(plan.rows, plan.phases * width)
    packed = jnp.pad(packed, ((0, 0), (0, plan.lanes - plan.phases * width)))
    basis, diag, off = lanczos(plan, near, packed)
    return covariance, basis, diag[1:], off


def solution(mesh):
    placed = (P(None, "tm"), P(("tm", "panel"), None))
    return jax.shard_map(
        local,
        mesh=mesh,
        in_specs=placed,
        out_specs=(P(("tm", "panel"), None), P(None, ("tm", "panel"), None), P(), P()),
        check_vma=False,
    )
```

```python
import jax
import jax.numpy as jnp
from jax import lax
from jax.experimental import pallas as pl
from jax.experimental.pallas import tpu as pltpu
from jax.sharding import PartitionSpec as P

M = 384
ITERS = 6
MESH = pl.DeviceIdType.MESH
EXACT = lax.Precision.HIGHEST
F32 = jnp.float32
BF16 = jnp.bfloat16
VMEM = pl.BlockSpec(memory_space=pltpu.VMEM)


def flip(index, mask):
    bit = 1
    while bit <= mask:
        if mask & bit:
            index = index + bit - 2 * bit * ((index // bit) % 2)
        bit *= 2
    return index


def round_up(value, unit):
    return -(-value // unit) * unit


class Plan:
    def __init__(self, channels, days, width, tm_size, panel_size):
        self.channels = channels
        self.days = days
        self.width = width
        self.tm_size = tm_size
        self.panel_size = panel_size
        self.lags = M // (tm_size * panel_size)
        self.phases = max(r for r in (1, 2, 3, 4) if self.lags % r == 0)
        self.groups = 8 if (8 * self.phases) % 16 == 0 else 16
        self.run = self.lags * panel_size
        self.pad = round_up(self.run + 2 * self.lags, self.groups * self.phases)
        self.reach = round_up(M + self.pad + self.lags, (16 // self.groups) * 32)
        self.reach = round_up(self.reach, self.groups * self.phases)
        self.units = self.reach // self.phases
        self.steps = self.units // self.groups
        self.together = 2 if self.steps % 2 == 0 and 2 * self.groups * channels <= 768 else 1
        self.depth = days + 128
        self.heads = self.lags // self.phases
        self.rows = self.heads * channels
        self.lanes = 128 * ((self.phases * width + 127) // 128)
        self.columns = tm_size // 2
        self.halves = panel_size // 2

    def offset(self, tm, panel):
        return (tm // 2) * 2 * self.run + panel * self.lags + self.pad


def series_kernel(size, s_ref, o_ref, held, send_sem, recv_sem):
    me = lax.axis_index("tm")
    days = s_ref.shape[1]
    barrier = pltpu.get_barrier_semaphore()
    for distance in range(1, size):
        pl.semaphore_signal(
            barrier, inc=1, device_id={"tm": (me + distance) % size}, device_id_type=MESH
        )
    pl.semaphore_wait(barrier, size - 1)
    copies = []
    for distance in range(1, size):
        copy = pltpu.make_async_remote_copy(
            src_ref=s_ref,
            dst_ref=held.at[distance],
            send_sem=send_sem.at[distance],
            recv_sem=recv_sem.at[distance],
            device_id={"tm": (me + distance) % size},
            device_id_type=MESH,
        )
        copy.start()
        copies.append(copy)
    o_ref[me] = s_ref[...]
    for distance, copy in enumerate(copies, 1):
        copy.wait_recv()
        o_ref[(me + size - distance) % size] = held[distance]
    for copy in copies:
        copy.wait_send()


def all_days(series, size):
    return pl.pallas_call(
        lambda *refs: series_kernel(size, *refs),
        out_shape=jax.ShapeDtypeStruct((size,) + series.shape, F32),
        in_specs=[VMEM],
        out_specs=VMEM,
        scratch_shapes=[
            pltpu.VMEM((size,) + series.shape, F32),
            pltpu.SemaphoreType.DMA((size,)),
            pltpu.SemaphoreType.DMA((size,)),
        ],
        compiler_params=pltpu.CompilerParams(collective_id=0, has_side_effects=True),
    )(series)


def covariance_kernel(
    plan, d_ref, n_ref, near_ref, c_ref, xh_ref, xl_ref, gh_ref, gl_ref, moved, woven, wide, sem
):
    channels, phases = plan.channels, plan.phases
    unit = plan.groups * channels
    tm, panel = lax.axis_index("tm"), lax.axis_index("panel")
    length = moved.shape[1]
    for n in range(d_ref.shape[0]):
        moved[:, n * d_ref.shape[2] : (n + 1) * d_ref.shape[2]] = d_ref[n]
    moved[:, plan.days :] = jnp.zeros((channels, length - plan.days), F32)
    for p in range(phases):
        rows = slice(p * channels, (p + 1) * channels)
        shifted = moved[:, : plan.depth]
        if p:
            shifted = pltpu.roll(shifted, p, 1)
        high = shifted.astype(BF16)
        xh_ref[rows, :] = high
        xl_ref[rows, :] = (shifted - high.astype(F32)).astype(BF16)
    moved[...] = pltpu.roll(moved[...], plan.offset(tm, panel), 1)

    def transpose(step, carry):
        at = pl.multiple_of(step * 128, 128)
        window = moved[:, pl.ds(at, 256)]
        stack = [window[:, phases * g : phases * g + 128] for g in range(plan.groups)]
        block = jnp.concatenate(stack, axis=0).T
        high = block.astype(BF16)
        gh_ref[pl.ds(at, 128), :] = high
        gl_ref[pl.ds(at, 128), :] = (block - high.astype(F32)).astype(BF16)
        return carry

    lax.fori_loop(0, gh_ref.shape[0] // 128, transpose, 0)
    together = plan.together

    span = together * unit * phases
    core = tm % 2
    jump = plan.run * channels
    behind = -(-plan.pad * channels // span)
    pieces = M * channels // span
    rows_of = []
    shifts = {}
    for i in range(plan.lags):
        first = (plan.pad - i) * channels
        if jump % 128:
            first = first - jump * core
            start = (first - 1) // 128 * 128
            shift = first - start
        else:
            start = (first - 1) // 128 * 128
            shift = first - start
            start = start - jump * core
        slot = shifts.setdefault((plan.pad - i) * channels % 128, (len(shifts), shift))[0]
        rows_of.append((slot, start))
    woven[...] = jnp.zeros(woven.shape, F32)

    def row_copy(i, q):
        slot, start = rows_of[i]
        at = pl.multiple_of(start + 128 + span * q, 128)
        to = pl.multiple_of(span * q, 128)
        return pltpu.make_async_copy(
            wide.at[slot, :, pl.ds(at, span)],
            c_ref.at[pl.ds(i * channels, channels), pl.ds(to, span)],
            sem.at[i, q],
        )

    def turn(step):
        to = pl.ds(pl.multiple_of(step * span, 128), span)
        for group in range(channels // 8):
            rows = slice(group * 8, group * 8 + 8)
            whole = woven[rows, :]
            for slot, shift in shifts.values():
                wide[slot, rows, to] = pltpu.roll(whole, span + 128 - shift, 1)[:, :span]

    def send_rows(step):
        @pl.when((step >= behind) & (step < behind + pieces))
        def _():
            for i in range(plan.lags):
                row_copy(i, step - behind).start()

    def product(step, carry):
        turn(jnp.maximum(step - 1, 0))
        pieces_h, pieces_l = [], []
        for g in range(together):
            start = pl.multiple_of((step * together + g) * plan.groups * phases, 16)
            pieces_h.append(gh_ref[pl.ds(start, plan.depth), :])
            pieces_l.append(gl_ref[pl.ds(start, plan.depth), :])
        high = jnp.concatenate(pieces_h, axis=1) if together > 1 else pieces_h[0]
        low = jnp.concatenate(pieces_l, axis=1) if together > 1 else pieces_l[0]
        total = jnp.dot(xh_ref[...], high, preferred_element_type=F32)
        total += jnp.dot(xh_ref[...], low, preferred_element_type=F32)
        total += jnp.dot(xl_ref[...], high, preferred_element_type=F32)
        at = pl.ds(pl.multiple_of(step * together * unit, 128), together * unit)
        counts = n_ref[:, at]
        for p in range(phases):
            rows = slice(p * channels, (p + 1) * channels)
            near_ref[rows, at] = total[rows] / counts[p : p + 1]

        woven[:, :128] = woven[:, span:]
        for t in range(together):
            start = pl.multiple_of((step * together + t) * unit, 128)
            block = near_ref[:, pl.ds(start, unit)]
            parts = [
                block[p * channels : (p + 1) * channels, g * channels : (g + 1) * channels]
                for g in range(plan.groups)
                for p in range(phases)
            ]
            to = 128 + t * unit * phases
            woven[:, to : to + unit * phases] = jnp.concatenate(parts, axis=1)
        send_rows(step - 1)
        return carry

    last = plan.steps // together
    lax.fori_loop(0, last, product, 0)
    turn(last - 1)
    send_rows(last - 1)
    for q in range(pieces):
        for i in range(plan.lags):
            row_copy(i, q).wait()


def covariance_rows(plan, days_by_device):
    channels, phases, days = plan.channels, plan.phases, plan.days
    base = -plan.offset(lax.axis_index("tm"), lax.axis_index("panel"))
    stretch = round_up(plan.depth + plan.groups * phases * (plan.steps - 1), 128)
    lag = base + jnp.arange(plan.units * channels) // channels * phases
    lag = lag[None, :] + jnp.arange(phases)[:, None]
    counts = (days - jnp.abs(lag)).astype(F32)
    shifts = len({(plan.pad - i) * channels % 128 for i in range(plan.lags)})
    span = plan.together * plan.groups * phases * channels
    return pl.pallas_call(
        lambda *refs: covariance_kernel(plan, *refs),
        out_shape=(
            jax.ShapeDtypeStruct((phases * channels, plan.units * channels), F32),
            jax.ShapeDtypeStruct((plan.lags * channels, M * channels), F32),
        ),
        in_specs=[VMEM] * 2,
        out_specs=(VMEM, pl.BlockSpec(memory_space=pl.ANY)),
        scratch_shapes=[
            pltpu.VMEM((phases * channels, plan.depth), BF16),
            pltpu.VMEM((phases * channels, plan.depth), BF16),
            pltpu.VMEM((stretch, plan.groups * channels), BF16),
            pltpu.VMEM((stretch, plan.groups * channels), BF16),
            pltpu.VMEM((channels, max(stretch + 128, days + plan.reach)), F32),
            pltpu.VMEM((channels, span + 128), F32),
            pltpu.VMEM((shifts, channels, plan.reach * channels), F32),
            pltpu.SemaphoreType.DMA((plan.lags, M * channels // span)),
        ],
        compiler_params=pltpu.CompilerParams(vmem_limit_bytes=60 * 1024 * 1024),
    )(days_by_device, counts)


def factor_and_inverse(gram, width):
    lanes = 2 * width
    row = lax.broadcasted_iota(jnp.int32, (width, lanes), 0)
    lane = lax.broadcasted_iota(jnp.int32, (width, lanes), 1)
    work = jnp.where(lane < width, gram, jnp.where(lane - width == row, 1.0, 0.0))
    for j in range(width):
        pivot_row = work[j : j + 1, :]
        scale = lax.rsqrt(jnp.broadcast_to(pivot_row[:, j : j + 1], (1, lanes)))
        pivot_row = pivot_row * scale
        column = jnp.broadcast_to(work[:, j : j + 1], (width, lanes)) * scale
        work = jnp.where(row > j, work - column * pivot_row, jnp.where(row == j, pivot_row, work))
    return jnp.where((lane < width) & (lane < row), 0.0, work)


def lanczos_kernel(
    plan,
    near_ref,
    x_ref,
    basis_ref,
    diag_ref,
    off_ref,
    left,
    zg,
    right,
    parts,
    q_s,
    z_s,
    v_s,
    guess,
    y_send,
    y_recv,
    g_held,
    g_got,
    p_send,
    p_recv,
    c_send,
    c_recv,
    g_send,
    g_recv,
    y_sems,
):
    channels, phases, width = plan.channels, plan.phases, plan.width
    heads, rows, lanes = plan.heads, plan.rows, plan.lanes
    panel_size, columns, halves = plan.panel_size, plan.columns, plan.halves
    tm, panel = lax.axis_index("tm"), lax.axis_index("panel")
    core, k = tm % 2, tm // 2
    side, half = panel % 2, panel // 2
    bits = columns.bit_length() - 1

    gram_stages = [[("tm", flip(tm, 1))]]
    gram_stages.append([("tm", flip(tm, 2 * m)) for m in range(1, columns)])
    gram_stages.append([("panel", flip(panel, d)) for d in range(1, panel_size)])
    partners = [partner for stage in gram_stages for partner in stage]
    barrier = pltpu.get_barrier_semaphore()
    for axis, other in partners:
        pl.semaphore_signal(barrier, inc=1, device_id={axis: other}, device_id_type=MESH)

    zero = jnp.zeros((rows, lanes), F32)
    q_s[...] = zero
    v_s[...] = zero
    z_s[...] = x_ref[...]
    guess[...] = jnp.zeros_like(guess)
    zg[0, k, half] = x_ref[...]
    pl.semaphore_wait(barrier, len(partners))

    lane1 = lax.broadcasted_iota(jnp.int32, (width, 2 * width), 1)

    def spread(pair):
        low = jnp.where(lane1 < width, pair, 0.0)
        high = pltpu.roll(low, width, 1)
        none = jnp.zeros_like(low)
        out = []
        for p in range(lanes // width):
            here = low if p % 2 == 0 else high
            if p >= phases:
                here = none
            line = [here if t == p // 2 else none for t in range(lanes // (2 * width))]
            out.append(jnp.concatenate(line, axis=1) if len(line) > 1 else line[0])
        return jnp.concatenate(out, axis=0)

    def folded(square):
        even = odd = None
        for p in range(phases):
            block = square[p * width : (p + 1) * width, (p // 2) * 2 * width :][:, : 2 * width]
            if p % 2 == 0:
                even = block if even is None else even + block
            else:
                odd = block if odd is None else odd + block
        if odd is not None:
            even = even + pltpu.roll(odd, width, 1)
        return even

    def times(a, b):
        return jnp.dot(a, b, precision=EXACT, preferred_element_type=F32)

    def times_t(a, b):
        return lax.dot_general(
            a, b, (((1,), (1,)), ((), ())), precision=EXACT, preferred_element_type=F32
        )

    def t_times(a, b):
        return lax.dot_general(
            a, b, (((0,), (0,)), ((), ())), precision=EXACT, preferred_element_type=F32
        )

    def remote(src, dst, send, recv, axis, other):
        return pltpu.make_async_remote_copy(
            src_ref=src,
            dst_ref=dst,
            send_sem=send,
            recv_sem=recv,
            device_id={axis: other},
            device_id_type=MESH,
        )

    def panel_copy(par, d):
        slot = zg.at[par, k, half]
        other = flip(panel, 2 * d)
        return remote(slot, slot, p_send.at[par, d], p_recv.at[par, d], "panel", other)

    def panel_arrival(par, d):
        slot = zg.at[par, k, flip(half, d)]
        other = flip(panel, 2 * d)
        return remote(slot, slot, p_send.at[par, d], p_recv.at[par, d], "panel", other)

    orders = {}
    for d in range(halves):
        order = list(range(bits))
        orders[d] = order if d < (halves + 1) // 2 else order[::-1]

    def column_copy(par, mask, d, bit):
        slot = zg.at[par, flip(k, mask), flip(half, d)]
        n = (mask ^ (1 << bit)) * halves + d
        return remote(
            slot, slot, c_send.at[par, n], c_recv.at[par, n], "tm", flip(tm, 2 << bit)
        )

    def column_arrival(par, mask, d):
        order = orders[d]
        bit = [b for b in order if mask & (1 << b)][-1]
        slot = zg.at[par, flip(k, mask), flip(half, d)]
        n = mask * halves + d
        return remote(
            slot, slot, c_send.at[par, n], c_recv.at[par, n], "tm", flip(tm, 2 << bit)
        )

    def last_stage(mask, d):
        return max([s for s, b in enumerate(orders[d]) if mask & (1 << b)], default=-1)

    def gram_copies(par, s):
        first = sum(len(stage) for stage in gram_stages[:s])
        return [
            remote(
                g_held.at[par, s],
                g_got.at[par, first + n],
                g_send.at[par, first + n],
                g_recv.at[par, first + n],
                axis,
                other,
            )
            for n, (axis, other) in enumerate(gram_stages[s])
        ]

    def gram_send(par, s):
        copies = gram_copies(par, s)
        for copy in copies:
            copy.start()
        return copies

    def local_gram(par):
        z = z_s[...]
        both = t_times(jnp.concatenate([q_s[...], z], axis=1), z)
        first = folded(both[:lanes])
        second = folded(both[lanes:])
        g_held[par, 0] = jnp.where(lane1 < width, first, pltpu.roll(second, width, 1))
        return gram_send(par, 0)

    def gram_stage(par, s, copies):
        first = sum(len(stage) for stage in gram_stages[:s])
        terms = [g_held[par, s]]
        for n, copy in enumerate(copies):
            copy.wait_recv()
            terms.append(g_got[par, first + n])
        while len(terms) > 1:
            terms = [terms[n] + terms[n + 1] for n in range(0, len(terms), 2)]
        g_held[par, s + 1] = terms[0]
        return gram_send(par, s + 1) if s + 1 < len(gram_stages) else []

    def small(par, j):
        both = g_held[par, len(gram_stages)]
        rest = jnp.where(lane1 < width, both, 0.0)
        square = t_times(rest, rest)[:width]
        gram = pltpu.roll(both, width, 1) - square
        work = factor_and_inverse(gram, width)
        diag = rest + guess[...]
        diag_ref[j] = diag[:, :width]
        off_ref[j] = work[:, :width]
        spread_rest = spread(rest)
        spread_r = spread(work)
        spread_l = spread(pltpu.roll(work, width, 1))
        products = times(jnp.concatenate([q_s[...], v_s[...]], axis=0), spread_rest)
        after = z_s[...] - products[:rows]
        following = times_t(after, spread_l)
        for p in range(phases):
            block = following[:, (p // 2) * 2 * width :][:, : 2 * width]
            if p % 2:
                block = pltpu.roll(block, width, 1)
            for h in range(heads):
                basis_ref[j, pl.ds((h * phases + p) * channels, channels), :] = block[
                    h * channels : (h + 1) * channels, :width
                ]
        return diag, products[rows:], spread_r, spread_l, following

    def build(same_core, same_side):
        total = plan.units * channels
        ahead = side if same_side else 3 * side - 1
        ahead = ahead * heads
        if not same_core:
            ahead = ahead + (2 * core - 1) * (plan.run // phases)
        turn = (total - ahead * channels) % total
        variant = 2 * int(same_core) + int(same_side)
        stride = 2 * plan.run // phases * channels
        piece = heads * channels
        for p in range(phases):

            def chunk(c, carry):
                at = pl.multiple_of(p * channels + c * 16, 16)
                part = pltpu.roll(near_ref[pl.ds(at, 16), :], turn, 1)
                for i in range(1 - phases, plan.lags):
                    if (plan.pad - i - p) % phases:
                        continue
                    u0 = (plan.pad - i - p) // phases
                    to = pl.ds(pl.multiple_of((i + phases - 1) * channels + c * 16, 16), 16)
                    for h in range(halves):
                        pieces = []
                        for n in range(columns):
                            start = u0 * channels + n * stride + 2 * h * piece
                            pieces.append(part[:, start : start + piece])
                        line = jnp.concatenate(pieces, axis=1)
                        high = line.astype(BF16)
                        low = (line - high.astype(F32)).astype(BF16)
                        depth = line.shape[1]
                        left[variant, h, to, :depth] = high
                        left[variant, h, to, depth : 2 * depth] = high
                        left[variant, h, to, 2 * depth :] = low
                return carry

            lax.fori_loop(0, channels // 16, chunk, 0)

    def add_product(variant, which, first):
        total = jnp.dot(left[variant, which], right[which], preferred_element_type=F32)
        parts[variant] = total if first else parts[variant] + total

    def combined(variant):
        lane = lax.broadcasted_iota(jnp.int32, (channels, lanes), 1)
        out = []
        for h in range(heads):
            total = None
            for delta in range(1 - phases, phases):
                i = h * phases + delta + phases - 1
                term = parts[variant, i * channels : (i + 1) * channels, :]
                if delta:
                    term = pltpu.roll(term, (delta * width) % lanes, 1)
                    if delta > 0:
                        keep = lane >= delta * width
                    else:
                        keep = lane < (phases + delta) * width
                    term = jnp.where(keep, term, 0.0)
                total = term if total is None else total + term
            out.append(total)
        whole = jnp.concatenate(out, axis=0) if heads > 1 else out[0]
        if phases * width < lanes:
            whole = jnp.where(
                lax.broadcasted_iota(jnp.int32, whole.shape, 1) < phases * width, whole, 0.0
            )
        return whole

    def take_in(par, mask, d):
        column = flip(k, mask)
        block = zg[par, column, flip(half, d)]
        high = block.astype(BF16)
        low = (block - high.astype(F32)).astype(BF16)
        for n, term in enumerate((high, low, high)):
            to = pl.ds(pl.multiple_of((n * columns + column) * rows, 16), rows)
            right[flip(half, d), to, :] = term

    events = [(2.0, "gram", 0), (6.5, "gram", 1), (13.0, "gram", 2), (13.5, "small", 0)]
    events.append((9.5, "products", 0))
    events.append((0.5, "build", (False, False)))
    events.append((2.5, "build", (False, True)))
    events.append((7.1, "build", (True, False)))
    events.append((7.2, "build", (True, True)))
    for d in range(halves):
        if d:
            events.append((7.0 * d, "panel", d))
        for mask in range(1, columns):
            if last_stage(mask, d) < bits - 1:
                hops = bin(mask).count("1")
                events.append((7.0 * d + 4.5 * hops, "column", (mask, d)))
    events.sort(key=lambda event: event[0])

    def iteration(j, carry):
        par = j % 2
        sends = []

        def forward(mask, d):
            for bit in orders[d][last_stage(mask, d) + 1 :]:
                copy = column_copy(par, mask, d, bit)
                copy.start()
                sends.append(copy)

        def arrive(mask, d):
            arrival = column_arrival(par, mask, d) if mask else panel_arrival(par, d)
            arrival.wait_recv()
            forward(mask, d)
            take_in(par, mask, d)
            arrived.add((mask, d))

        def arrive_half(d):
            for mask in range(columns):
                if (mask, d) not in arrived:
                    arrive(mask, d)

        for d in range(1, halves):
            copy = panel_copy(par, d)
            copy.start()
            sends.append(copy)
        forward(0, 0)

        gram = local_gram(par)
        sends += gram
        take_in(par, 0, 0)
        arrived = {(0, 0)}
        for _, kind, what in events:
            if kind == "gram":
                gram = gram_stage(par, what, gram)
                sends += gram
            elif kind == "small":
                diag, v_part, spread_r, spread_l, following = small(par, j)
                q_r = times_t(q_s[...], spread_r) + times(following, spread(diag))
            elif kind == "build":

                @pl.when(j == 0)
                def _():
                    build(*what)

            elif kind == "products":
                for d in range(halves - 1):
                    arrive_half(d)
                    for variant in range(4):
                        add_product(variant, flip(half, d), d == 0)
            elif kind == "panel":
                arrive(0, what)
            else:
                arrive(*what)
        guess[...] = diag
        last = halves - 1
        arrive_half(last)
        across = {}

        def to_core(other_side):
            variant = 1 - other_side
            add_product(variant, flip(half, last), last == 0)
            y_send[par, other_side] = combined(variant)
            copy = remote(
                y_send.at[par, other_side],
                y_recv.at[par, other_side],
                y_sems.at[par, other_side],
                y_sems.at[par, 2 + other_side],
                "tm",
                flip(tm, 1),
            )
            copy.start()
            across[other_side] = copy

        to_core(1)
        add_product(2, flip(half, last), last == 0)
        near_side = combined(2)
        across[1].wait_recv()
        y_send[par, 2] = near_side + y_recv[par, 1]
        over = remote(
            y_send.at[par, 2],
            y_recv.at[par, 2],
            y_sems.at[par, 4],
            y_sems.at[par, 5],
            "panel",
            flip(panel, 1),
        )
        over.start()
        to_core(0)
        add_product(3, flip(half, last), last == 0)
        mine = combined(3) - v_part
        across[0].wait_recv()
        mine = mine + y_recv[par, 0]
        over.wait_recv()
        v = times_t(mine + y_recv[par, 2], spread_l)
        z = v - q_r
        v_s[...] = v
        z_s[...] = z
        q_s[...] = following
        zg[1 - par, k, half] = z
        for copy in sends + [across[0], across[1], over]:
            copy.wait_send()
        return carry

    lax.fori_loop(0, ITERS, iteration, 0)
    par = ITERS % 2
    gram = local_gram(par)
    sends = list(gram)
    for s in range(len(gram_stages)):
        gram = gram_stage(par, s, gram)
        sends += gram
    small(par, ITERS)
    for copy in sends:
        copy.wait_send()


def lanczos(plan, near, packed):
    channels, phases, width = plan.channels, plan.phases, plan.width
    rows, lanes = plan.rows, plan.lanes
    blocks = plan.columns * plan.halves
    groups = (plan.lags + phases - 1) * channels
    others = plan.columns + plan.panel_size - 1
    block = (rows, lanes)
    pair = (width, 2 * width)
    dma = pltpu.SemaphoreType.DMA
    return pl.pallas_call(
        lambda *refs: lanczos_kernel(plan, *refs),
        out_shape=(
            jax.ShapeDtypeStruct((ITERS + 1, plan.lags * channels, width), F32),
            jax.ShapeDtypeStruct((ITERS + 1, width, width), F32),
            jax.ShapeDtypeStruct((ITERS + 1, width, width), F32),
        ),
        in_specs=[VMEM] * 2,
        out_specs=(VMEM,) * 3,
        scratch_shapes=[
            pltpu.VMEM((4, plan.halves, groups, 3 * plan.columns * rows), BF16),
            pltpu.VMEM((2, plan.columns, plan.halves) + block, F32),
            pltpu.VMEM((plan.halves, 3 * plan.columns * rows, lanes), BF16),
            pltpu.VMEM((4, groups, lanes), F32),
            pltpu.VMEM(block, F32),
            pltpu.VMEM(block, F32),
            pltpu.VMEM(block, F32),
            pltpu.VMEM(pair, F32),
            pltpu.VMEM((2, 3) + block, F32),
            pltpu.VMEM((2, 3) + block, F32),
            pltpu.VMEM((2, 4) + pair, F32),
            pltpu.VMEM((2, others) + pair, F32),
            dma((2, plan.halves)),
            dma((2, plan.halves)),
            dma((2, blocks)),
            dma((2, blocks)),
            dma((2, others)),
            dma((2, others)),
            dma((2, 6)),
        ],
        compiler_params=pltpu.CompilerParams(
            collective_id=1, has_side_effects=True, vmem_limit_bytes=60 * 1024 * 1024
        ),
    )(near, packed)


def local(series, start_block):
    channels, day_count = series.shape
    tm_size = lax.axis_size("tm")
    panel_size = lax.axis_size("panel")
    width = start_block.shape[1]
    plan = Plan(channels, day_count * tm_size, width, tm_size, panel_size)
    near, covariance = covariance_rows(plan, all_days(series, tm_size))
    packed = start_block.reshape(plan.heads, plan.phases, channels, width)
    packed = jnp.transpose(packed, (0, 2, 1, 3)).reshape(plan.rows, plan.phases * width)
    packed = jnp.pad(packed, ((0, 0), (0, plan.lanes - plan.phases * width)))
    basis, diag, off = lanczos(plan, near, packed)
    return covariance, basis, diag[1:], off


def solution(mesh):
    placed = (P(None, "tm"), P(("tm", "panel"), None))
    return jax.shard_map(
        local,
        mesh=mesh,
        in_specs=placed,
        out_specs=(P(("tm", "panel"), None), P(None, ("tm", "panel"), None), P(), P()),
        check_vma=False,
    )
```
